32 devices in a mesh: owner: 8 (over y, x, core), rows: 4 (over z).
Axes of the slice: x: 2, y: 2, z: 4, core: 2. Of those that a mesh axis runs over, the one named last changes fastest.
Arguments:
- w_down: float32 [64, 1408, 2048], P('owner', None, 'rows'), may hold values from -0.21875 to 0.21875
- router_weight: float32 [2048, 64], P('rows', 'owner'), may hold values from -0.125 to 0.125
- router_gain: float32 [2048], P('rows'), may hold values from 0.25 to 1.75
Outputs:
- serve_down: bfloat16 [64, 1408, 2048], P('owner')
- scale_down: float32 [64, 1408], P('owner')
- serve_router: bfloat16 [2048, 64], replicated
The draws below stay inside these ranges and needn't reach their ends.
All inputs are finite; a program needn't handle non-finite values. Where the reference program divides by a largest or mean magnitude, that divisor is 1e-20 or more.
Results may differ from the reference program's by a relative error of at most 0.001.
Values may be sent and summed in bfloat16 or wider, within the bound.
A program may use at most 192 MiB of HBM per device.

```python
import jax
import jax.numpy as jnp

EXPERTS = 64
D_MODEL = 2048
D_EXPERT = 1408


def raised(result, stream_key, source, target, parts, factor):
    owner, partner = [(jnp.arange(result.shape[dim]) // (result.shape[dim] // parts)).reshape([-1 if axis == dim else 1 for axis in range(result.ndim)]) for dim in (source, target)]
    chosen = jax.random.permutation(stream_key, parts)[partner]
    strong = (owner == chosen) | (owner == (partner + parts // 2) % parts)
    return jnp.where(strong, factor * result, result)


def levels(own_key, shape, split, low, high):
    gain = 1.0
    for axis_at, parts in split:
        draws = jax.random.uniform(jax.random.fold_in(jax.random.fold_in(own_key, 6), axis_at), (parts,), jnp.float32, low / len(split), high / len(split))
        gain = gain * jnp.repeat(jnp.exp(draws), shape[axis_at] // parts).reshape((-1,) + (1,) * (len(shape) - 1 - axis_at))
    return gain


def gaussian(rng, extent, deviation, reach, cuts=(), held_as=jnp.bfloat16):
    factor_of = levels(rng, extent, cuts, -0.22, 0.18) if cuts else 1.0
    drawn = jax.random.normal(rng, extent, jnp.float32) * deviation * factor_of
    return jnp.minimum(jnp.maximum(drawn, -reach), reach).astype(held_as)


def gaussian_with(own_key, extent, scale, limit, pieces, heavy, held_as=jnp.bfloat16):
    entries = scale * jax.random.normal(own_key, extent, jnp.float32)
    if pieces:
        entries = entries * levels(own_key, extent, pieces, -0.22, 0.18)
    return jnp.clip(raised(entries, jax.random.fold_in(own_key, 3), *heavy), -limit, limit).astype(held_as)


def setup_inputs(seed: int = 0) -> dict:
    seeds = jax.random.split(jax.random.key(seed), 4)
    return {
        "w_down": gaussian_with(seeds[0], (EXPERTS, D_EXPERT, D_MODEL), D_EXPERT ** -0.5, 0.21875, ((0, 8), (2, 4)), (2, 1, 4, 2.0), jnp.float32),
        "router_weight": gaussian(seeds[1], (D_MODEL, EXPERTS), D_MODEL ** -0.5, 0.125, ((0, 4), (1, 8)), jnp.float32),
        "router_gain": jnp.clip(1.0 + 0.15 * jax.random.normal(seeds[2], (D_MODEL,), jnp.float32), 0.25, 1.75),
    }


def reference(w_down, router_weight, router_gain):
    scale_down = jnp.max(jnp.abs(w_down), axis=2)
    serve_down = (w_down / jnp.expand_dims(scale_down, 2)).astype(jnp.bfloat16)
    serve_router = (router_weight * router_gain[:, None]).astype(jnp.bfloat16)
    return serve_down, scale_down, serve_router
```

```python
import functools

import jax
import jax.numpy as jnp
from jax import lax
from jax.experimental import pallas as pl
from jax.experimental.pallas import tpu as pltpu
from jax.sharding import PartitionSpec as P


LANES = 128
TAIL = 384


def tile_max(ref, e, r):
    block = jnp.abs(ref[e, pl.ds(r, LANES), :LANES])
    for c in range(LANES, ref.shape[2], LANES):
        block = jnp.maximum(block, jnp.abs(ref[e, pl.ds(r, LANES), c : c + LANES]))
    return jnp.max(block.T, axis=0, keepdims=True)


def normalise(values, scales):
    per_row = jnp.broadcast_to(scales, (LANES, LANES)).T
    parts = [values[:, c : c + LANES] / per_row for c in range(0, values.shape[1], LANES)]
    return jnp.concatenate(parts, axis=1).astype(jnp.bfloat16)


def head_kernel(sizes, w_hbm, weight_ref, gain_ref, scale_ref, own_ref, table_ref, held, peak, w_sem, peak_send, peak_recv, row_send, row_recv, all_send, all_recv):
    owners, n = sizes
    experts, depth, _ = w_hbm.shape
    me, mine = lax.axis_index("rows"), lax.axis_index("owner")
    loads = [pltpu.make_async_copy(w_hbm.at[e], held.at[e], w_sem.at[e]) for e in range(experts)]
    for load in loads:
        load.start()

    barrier = pltpu.get_barrier_semaphore()
    for k in range(1, n):
        pl.semaphore_signal(barrier, inc=1, device_id={"rows": lax.rem(me + k, n)}, device_id_type=pl.DeviceIdType.MESH)
    for k in range(1, owners):
        pl.semaphore_signal(barrier, inc=1, device_id={"owner": lax.rem(mine + k, owners)}, device_id_type=pl.DeviceIdType.MESH)
    table_ref[mine, me] = (weight_ref[...] * gain_ref[...]).astype(jnp.bfloat16)
    pl.semaphore_wait(barrier, n - 1 + owners - 1)

    def reduce_expert(e):
        loads[e].wait()
        for r in range(0, depth, LANES):
            peak[me, e : e + 1, r : r + LANES] = tile_max(held, e, r)

    def copies(k_range, ref, key, axis, here, size, send, recv):
        return [
            pltpu.make_async_remote_copy(
                src_ref=ref.at[key],
                dst_ref=ref.at[key],
                send_sem=send.at[k],
                recv_sem=recv.at[k],
                device_id={axis: lax.rem(here + k, size)},
                device_id_type=pl.DeviceIdType.MESH,
            )
            for k in k_range
        ]

    half = experts // 2
    reduce_expert(0)
    to_rows = copies(range(1, n), table_ref, (mine, me), "rows", me, n, row_send, row_recv)
    for copy in to_rows:
        copy.start()
    for e in range(1, half + 1):
        reduce_expert(e)
    for copy in to_rows:
        copy.wait()
    to_owners = copies(range(1, owners), table_ref, mine, "owner", mine, owners, all_send, all_recv)
    for copy in to_owners:
        copy.start()
    for e in range(half + 1, experts):
        reduce_expert(e)
    for copy in to_owners:
        copy.wait()
    to_peers = copies(range(1, n), peak, me, "rows", me, n, peak_send, peak_recv)
    for copy in to_peers:
        copy.start()
    for copy in to_peers:
        copy.wait()
    scale = peak[0]
    for k in range(1, n):
        scale = jnp.maximum(scale, peak[k])
    scale_ref[...] = scale
    for r in range(0, depth, LANES):
        own_ref[pl.ds(r, LANES), :] = normalise(held[0, pl.ds(r, LANES), :], scale_ref[0:1, r : r + LANES])


def head(w_down, router_weight, router_gain, owners, n):
    experts, depth, columns = w_down.shape
    width, share = router_weight.shape
    vmem = pl.BlockSpec(memory_space=pltpu.VMEM)
    dma = pltpu.SemaphoreType.DMA
    return pl.pallas_call(
        functools.partial(head_kernel, (owners, n)),
        out_shape=(
            jax.ShapeDtypeStruct((experts, depth), jnp.float32),
            jax.ShapeDtypeStruct((depth, columns), jnp.bfloat16),
            jax.ShapeDtypeStruct((owners, n, share, width), jnp.bfloat16),
        ),
        in_specs=[pl.BlockSpec(memory_space=pl.ANY), vmem, vmem],
        out_specs=(vmem, vmem, vmem),
        scratch_shapes=[
            pltpu.VMEM(w_down.shape, jnp.float32),
            pltpu.VMEM((n, experts, depth), jnp.float32),
            dma((experts,)),
            dma((n,)),
            dma((n,)),
            dma((n,)),
            dma((n,)),
            dma((owners,)),
            dma((owners,)),
        ],
        compiler_params=pltpu.CompilerParams(collective_id=0, has_side_effects=True, vmem_limit_bytes=48 * 2**20),
    )(w_down, router_weight.T, router_gain[None, :])


def norm_kernel(step_rows, w_ref, scale_ref, own_ref):
    for r in range(0, step_rows, LANES):
        own_ref[pl.ds(r, LANES), :] = normalise(w_ref[0, pl.ds(r, LANES), :], scale_ref[0, 0:1, r : r + LANES])


def norm(w_down, scales, e, row, rows):
    columns = w_down.shape[2]
    step_rows = LANES if row else rows
    at = row // step_rows
    return pl.pallas_call(
        functools.partial(norm_kernel, step_rows),
        out_shape=jax.ShapeDtypeStruct((rows, columns), jnp.bfloat16),
        grid=(rows // step_rows,),
        in_specs=[
            pl.BlockSpec((1, step_rows, columns), lambda r: (e, at + r, 0)),
            pl.BlockSpec((1, 1, step_rows), lambda r: (e, 0, at + r)),
        ],
        out_specs=pl.BlockSpec((step_rows, columns), lambda r: (r, 0)),
        cost_estimate=pl.CostEstimate(flops=rows * columns * 8, bytes_accessed=rows * columns * 6, transcendentals=0),
    )(w_down, scales)


def place_kernel(offsets, n, me_ref, *refs):
    out = refs[-1]
    for offset, block in zip(offsets, refs):
        slot = me_ref[0] + offset
        columns = block.shape[1]

        @pl.when((slot >= 0) & (slot < n))
        def _():
            out[0, :, pl.ds(pl.multiple_of(slot * columns, LANES), columns)] = block[...]


def place(me, blocks, serve, shape, e, row):
    rows, columns = blocks[0].shape
    n = shape[2] // columns
    step_rows = LANES if row else (rows // 2 if rows % 32 == 0 else rows)
    at = row // step_rows

    def spec(offset):
        def index(r, me_ref):
            slot = me_ref[0] + offset
            return jnp.where((slot >= 0) & (slot < n), r, 0), 0

        return pl.BlockSpec((step_rows, columns), index)

    first = serve is None
    return pl.pallas_call(
        functools.partial(place_kernel, tuple(blocks), n),
        out_shape=jax.ShapeDtypeStruct(shape, jnp.bfloat16),
        grid_spec=pltpu.PrefetchScalarGridSpec(
            num_scalar_prefetch=1,
            grid=(rows // step_rows,),
            in_specs=[spec(offset) for offset in blocks] + ([] if first else [pl.BlockSpec(memory_space=pl.ANY)]),
            out_specs=pl.BlockSpec((1, step_rows, shape[2]), lambda r, _: (e, at + r, 0)),
        ),
        input_output_aliases={} if first else {1 + len(blocks): 0},
        cost_estimate=pl.CostEstimate(flops=rows * columns * 64, bytes_accessed=rows * columns * 22, transcendentals=0),
    )(me, *blocks.values(), *([] if first else [serve]))


def plan(experts, depth):
    cut = depth - TAIL
    return [(e, 0, depth) for e in range(experts - 1)] + [(experts - 1, 0, cut), (experts - 1, cut, TAIL)]


def on_device(owners, n, w_down, router_weight, router_gain):
    me = lax.axis_index("rows")
    me_array = me.astype(jnp.int32).reshape((1,))
    experts, depth, columns = w_down.shape
    shape = (experts, depth, n * columns)
    scale_down, first, table = head(w_down, router_weight, router_gain, owners, n)
    scales = scale_down[:, None, :]
    chunks = plan(experts, depth)
    held = []
    serve = None
    for at in range(len(chunks) + n - 1):
        if at < len(chunks):
            held.append({0: first if at == 0 else norm(w_down, scales, *chunks[at])})
        for step in range(1, n):
            c = at - step + 1
            if 0 <= c < len(chunks):
                held[c][-step] = lax.ppermute(held[c][1 - step], "rows", [(i, i + 1) for i in range(step - 1, n - 1)])
                held[c][step] = lax.ppermute(held[c][step - 1], "rows", [(i + 1, i) for i in range(0, n - step)])
        c = at - n + 1
        if c >= 0:
            serve = place(me_array, held[c], serve, shape, *chunks[c][:2])
    serve_router = table.transpose(1, 3, 0, 2).reshape(n * table.shape[3], owners * table.shape[2])
    return (serve, scale_down, serve_router)


def solution(mesh):
    owners, n = mesh.shape["owner"], mesh.shape["rows"]
    placed = (P("owner", None, "rows"), P("rows", "owner"), P("rows"))
    return jax.shard_map(
        functools.partial(on_device, owners, n),
        mesh=mesh,
        in_specs=placed,
        out_specs=(P("owner", None, None), P("owner", None), P()),
        check_vma=False,
    )
```

```python
import functools

import jax
import jax.numpy as jnp
from jax import lax
from jax.experimental import pallas as pl
from jax.experimental.pallas import tpu as pltpu
from jax.sharding import PartitionSpec as P


LANES = 128
LEAD = 2
TAIL = 128


def tile_max(ref, e, r):
    block = jnp.abs(ref[e, pl.ds(r, LANES), :LANES])
    for c in range(LANES, ref.shape[2], LANES):
        block = jnp.maximum(block, jnp.abs(ref[e, pl.ds(r, LANES), c : c + LANES]))
    return jnp.max(block.T, axis=0, keepdims=True)


def normalise(values, scales):
    per_row = jnp.broadcast_to(scales, (LANES, LANES)).T
    parts = [values[:, c : c + LANES] / per_row for c in range(0, values.shape[1], LANES)]
    return jnp.concatenate(parts, axis=1).astype(jnp.bfloat16)


def to_all(ref, key, axis, here, size, sems):
    copies = [
        pltpu.make_async_remote_copy(
            src_ref=ref.at[key],
            dst_ref=ref.at[key],
            send_sem=sems.at[0, k],
            recv_sem=sems.at[1, k],
            device_id={axis: lax.rem(here + k, size)},
            device_id_type=pl.DeviceIdType.MESH,
        )
        for k in range(1, size)
    ]
    for copy in copies:
        copy.start()
    return copies


def wait(copies):
    for copy in copies:
        copy.wait()


def spread_kernel(owners, rows_ref, table_ref, load_sem, sems_all):
    mine = lax.axis_index("owner")
    load = pltpu.make_async_copy(rows_ref, table_ref.at[mine], load_sem)
    load.start()
    barrier = pltpu.get_barrier_semaphore()
    for k in range(1, owners):
        pl.semaphore_signal(barrier, inc=1, device_id={"owner": lax.rem(mine + k, owners)}, device_id_type=pl.DeviceIdType.MESH)
    pl.semaphore_wait(barrier, owners - 1)
    load.wait()
    wait(to_all(table_ref, mine, "owner", mine, owners, sems_all))


def spread(table, owners):
    return pl.pallas_call(
        functools.partial(spread_kernel, owners),
        out_shape=jax.ShapeDtypeStruct((owners,) + table.shape, jnp.float32),
        in_specs=[pl.BlockSpec(memory_space=pltpu.VMEM)],
        out_specs=pl.BlockSpec(memory_space=pltpu.VMEM),
        scratch_shapes=[pltpu.SemaphoreType.DMA, pltpu.SemaphoreType.DMA((2, owners))],
        compiler_params=pltpu.CompilerParams(collective_id=1, has_side_effects=True),
        cost_estimate=pl.CostEstimate(flops=table.size * 512, bytes_accessed=table.size * 64, transcendentals=0),
    )(table)


def head_kernel(sizes, early, w_hbm, weight_ref, gain_ref, scale_ref, own_ref, table_ref, held, peak, w_sem, sems_peak, sems_row):
    n = sizes
    lead, depth, _ = held.shape
    me = lax.axis_index("rows")
    mesh_ids = pl.DeviceIdType.MESH
    loads = [pltpu.make_async_copy(w_hbm.at[e], held.at[e], w_sem.at[e]) for e in range(lead)]
    for load in loads:
        load.start()

    barrier = pltpu.get_barrier_semaphore()
    for k in range(1, n):
        pl.semaphore_signal(barrier, inc=1, device_id={"rows": lax.rem(me + k, n)}, device_id_type=mesh_ids)
    table_ref[me] = weight_ref[...] * gain_ref[...]

    for e in range(lead):
        loads[e].wait()
        for r in range(0, depth, LANES):
            peak[me, e : e + 1, r : r + LANES] = tile_max(held, e, r)
    pl.semaphore_wait(barrier, n - 1)
    routes = to_all(table_ref, me, "rows", me, n, sems_row)
    tops = to_all(peak, me, "rows", me, n, sems_peak)
    wait(tops)
    scale = peak[0]
    for k in range(1, n):
        scale = jnp.maximum(scale, peak[k])
    scale_ref[...] = scale
    for r in range(0, early, LANES):
        own_ref[pl.ds(r, LANES), :] = normalise(held[0, pl.ds(r, LANES), :], scale_ref[0:1, r : r + LANES])
    wait(routes)


def head(w_down, router_weight, router_gain, n, lead, early):
    _, depth, columns = w_down.shape
    width, share = router_weight.shape
    vmem = pl.BlockSpec(memory_space=pltpu.VMEM)
    dma = pltpu.SemaphoreType.DMA
    return pl.pallas_call(
        functools.partial(head_kernel, n, early),
        out_shape=(
            jax.ShapeDtypeStruct((lead, depth), jnp.float32),
            jax.ShapeDtypeStruct((early, columns), jnp.bfloat16),
            jax.ShapeDtypeStruct((n, share, width), jnp.float32),
        ),
        in_specs=[pl.BlockSpec(memory_space=pl.ANY), vmem, vmem],
        out_specs=(vmem, vmem, vmem),
        scratch_shapes=[
            pltpu.VMEM((lead, depth, columns), jnp.float32),
            pltpu.VMEM((n, lead, depth), jnp.float32),
            dma((lead,)),
            dma((2, n)),
            dma((2, n)),
        ],
        compiler_params=pltpu.CompilerParams(collective_id=0, has_side_effects=True, vmem_limit_bytes=48 * 2**20),
    )(w_down, router_weight.T, router_gain[None, :])


def maxes_kernel(w_ref, peak_ref):
    for r in range(0, w_ref.shape[1], LANES):
        peak_ref[0, 0:1, r : r + LANES] = tile_max(w_ref, 0, r)


def maxes(w_down, lead):
    experts, depth, columns = w_down.shape
    return pl.pallas_call(
        maxes_kernel,
        out_shape=jax.ShapeDtypeStruct((experts - lead, 1, depth), jnp.float32),
        grid=(experts - lead,),
        in_specs=[pl.BlockSpec((1, depth, columns), lambda e: (e + lead, 0, 0))],
        out_specs=pl.BlockSpec((1, 1, depth), lambda e: (e, 0, 0)),
        cost_estimate=pl.CostEstimate(flops=w_down.size * 2, bytes_accessed=w_down.size * 4, transcendentals=0),
    )(w_down)


def small_kernel(*refs):
    *scale_refs, table_ref, scale_out, router_out, wide = refs
    row = 0
    for ref in scale_refs:
        for e in range(ref.shape[0]):
            scale_out[row : row + 1, :] = ref[e]
            row += 1
    owners, n, share, width = table_ref.shape
    for o in range(owners):
        for z in range(n):
            wide[o * share : (o + 1) * share, z * width : (z + 1) * width] = table_ref[o, z]
    router_out[...] = wide[...].astype(jnp.bfloat16)


def small(parts, table):
    owners, n, share, width = table.shape
    return pl.pallas_call(
        small_kernel,
        out_shape=(
            jax.ShapeDtypeStruct((sum(p.shape[0] for p in parts), parts[0].shape[2]), jnp.float32),
            jax.ShapeDtypeStruct((owners * share, n * width), jnp.bfloat16),
        ),
        scratch_shapes=[pltpu.VMEM((owners * share, n * width), jnp.float32)],
        cost_estimate=pl.CostEstimate(flops=table.size * 8, bytes_accessed=table.size * 6, transcendentals=0),
    )(*parts, table)


def norm_kernel(step_rows, w_ref, scale_ref, own_ref):
    for r in range(0, step_rows, LANES):
        own_ref[pl.ds(r, LANES), :] = normalise(w_ref[0, pl.ds(r, LANES), :], scale_ref[0, 0:1, r : r + LANES])


def norm(w_down, scales, e, row, rows, base):
    columns = w_down.shape[2]
    step_rows = LANES if row else rows
    at = row // step_rows
    return pl.pallas_call(
        functools.partial(norm_kernel, step_rows),
        out_shape=jax.ShapeDtypeStruct((rows, columns), jnp.bfloat16),
        grid=(rows // step_rows,),
        in_specs=[
            pl.BlockSpec((1, step_rows, columns), lambda r: (e, at + r, 0)),
            pl.BlockSpec((1, 1, step_rows), lambda r: (e - base, 0, at + r)),
        ],
        out_specs=pl.BlockSpec((step_rows, columns), lambda r: (r, 0)),
        cost_estimate=pl.CostEstimate(flops=rows * columns * 8, bytes_accessed=rows * columns * 6, transcendentals=0),
    )(w_down, scales)


def place_kernel(offsets, n, me_ref, *refs):
    out = refs[-1]
    for offset, block in zip(offsets, refs):
        slot = me_ref[0] + offset
        columns = block.shape[1]

        @pl.when((slot >= 0) & (slot < n))
        def _():
            out[0, :, pl.ds(pl.multiple_of(slot * columns, LANES), columns)] = block[...]


def place(me, blocks, serve, shape, e, row):
    rows, columns = blocks[0].shape
    n = shape[2] // columns
    step_rows = LANES if row else (rows // 2 if rows % 32 == 0 else rows)
    at = row // step_rows

    def spec(offset):
        def index(r, me_ref):
            slot = me_ref[0] + offset
            return jnp.where((slot >= 0) & (slot < n), r, 0), 0

        return pl.BlockSpec((step_rows, columns), index)

    first = serve is None
    return pl.pallas_call(
        functools.partial(place_kernel, tuple(blocks), n),
        out_shape=jax.ShapeDtypeStruct(shape, jnp.bfloat16),
        grid_spec=pltpu.PrefetchScalarGridSpec(
            num_scalar_prefetch=1,
            grid=(rows // step_rows,),
            in_specs=[spec(offset) for offset in blocks] + ([] if first else [pl.BlockSpec(memory_space=pl.ANY)]),
            out_specs=pl.BlockSpec((1, step_rows, shape[2]), lambda r, _: (e, at + r, 0)),
        ),
        input_output_aliases={} if first else {1 + len(blocks): 0},
        cost_estimate=pl.CostEstimate(flops=rows * columns * 64, bytes_accessed=rows * columns * 22, transcendentals=0),
    )(me, *blocks.values(), *([] if first else [serve]))


def plan(experts, depth):
    cut = depth - TAIL
    last = [(experts - 1, 0, cut), (experts - 1, cut, TAIL)]
    return [(e, 0, depth) for e in range(experts - 1)] + last


def on_device(owners, n, w_down, router_weight, router_gain):
    me = lax.axis_index("rows")
    me_array = me.astype(jnp.int32).reshape((1,))
    experts, depth, columns = w_down.shape
    shape = (experts, depth, n * columns)
    lead = min(LEAD, experts)
    scale_lead, first, table = head(w_down, router_weight, router_gain, n, lead, depth)
    scales = [scale_lead[:, None, :]]
    chunks = plan(experts, depth)
    held = []
    serve = None
    for at in range(len(chunks) + n - 1):
        if at < len(chunks):
            held.append({0: first if at == 0 else norm(w_down, scales[chunks[at][0] >= lead], *chunks[at], 0 if chunks[at][0] < lead else lead)})
        for step in range(1, n):
            c = at - step + 1
            if 0 <= c < len(chunks):
                held[c][-step] = lax.ppermute(held[c][1 - step], "rows", [(i, i + 1) for i in range(step - 1, n - 1)])
                held[c][step] = lax.ppermute(held[c][step - 1], "rows", [(i + 1, i) for i in range(0, n - step)])
        if at == 1 and experts > lead:
            tops = maxes(w_down, lead)
            scale = tops
            for k in range(1, n):
                scale = jnp.maximum(scale, lax.ppermute(tops, "rows", [(i, (i + k) % n) for i in range(n)]))
            scales.append(scale)
        c = at - n + 1
        if c >= 0:
            serve = place(me_array, held[c], serve, shape, *chunks[c][:2])
    table = spread(table, owners)
    scale_down, router = small(scales, table)
    return (serve, scale_down, router.T)


def solution(mesh):
    owners, n = mesh.shape["owner"], mesh.shape["rows"]
    placed = (P("owner", None, "rows"), P("rows", "owner"), P("rows"))
    return jax.shard_map(
        functools.partial(on_device, owners, n),
        mesh=mesh,
        in_specs=placed,
        out_specs=(P("owner", None, None), P("owner", None), P()),
        check_vma=False,
    )
```
